512 devices in a mesh: rows: 16 (over z, core), centres: 32 (over x, y).
Axes of the slice: x: 4, y: 8, z: 8, core: 2. Of those that a mesh axis runs over, the one named last changes fastest.
Arguments:
- features: bfloat16 [16384, 256], P('rows', 'centres'), may hold values from -11 to 11
- targets: bfloat16 [16384, 128], P('rows'), may hold values from -6 to 6
- centre_points: bfloat16 [16384, 256], P('centres'), may hold values from -11 to 11
- precond: bfloat16 [16384, 512], P('centres'), as said below
Outputs:
- coefficients: float32 [16384, 128], P('centres')
- fitted: float32 [16384, 128], P('rows')
The draws below stay inside these ranges and needn't reach their ends.
Inputs may be any that keep to these rules, and one draw needn't show every extreme that they name: Each diagonal block of 512 x 512 entries of precond is symmetric positive definite.
All inputs are finite; a program needn't handle non-finite values.
Results may differ from the reference program's by a relative error of at most 0.0076.
Values may be sent and summed in bfloat16 or wider, within the bound.
No kernel may reach another device: no remote copies, remote signals or barrier semaphores. Data moves between devices by JAX's collectives and lax.ppermute only.
A program may use at most 64 MiB of HBM per device.

```python
import jax
import jax.numpy as jnp
from jax import lax

D = 256
TARGETS = 128
ROW_DEV = 1024
CENTRE_DEV = 512
ITERS = 2
ROWS_ALL = 16384
CENTRES = 16384
N_CENTRES = 32


def cluster_means(key):
    groups = ROWS_ALL // ROW_DEV
    return jnp.clip(jax.random.normal(jax.random.fold_in(key, 101), (groups, D), jnp.float32), -4.0, 4.0)


def noise_draw(key, shape):
    values = jnp.clip(jax.random.normal(key, shape, jnp.float32), -4.0, 4.0)
    return values


def draw_features(key, part):
    means = cluster_means(key)
    groups = ROWS_ALL // ROW_DEV
    member = jax.random.randint(jax.random.fold_in(key, 404), (ROWS_ALL,), 0, groups, jnp.int32)
    noise = noise_draw(jax.random.fold_in(key, 202), (ROWS_ALL, D))
    return (1.7320508 * means[member] + noise).astype(jnp.bfloat16)


def draw_centre_points(key, part):
    means = cluster_means(key)
    groups = ROWS_ALL // ROW_DEV
    member = jax.random.randint(jax.random.fold_in(key, 505), (CENTRES,), 0, groups, jnp.int32)
    noise = noise_draw(jax.random.fold_in(key, 303), (CENTRES, D))
    return (1.7320508 * means[member] + noise).astype(jnp.bfloat16)


def draw_precond(key, part):
    block_total = CENTRES // CENTRE_DEV
    random_part = jax.random.normal(key, (block_total, CENTRE_DEV, CENTRE_DEV), jnp.float32)
    identity = jnp.eye(CENTRE_DEV, dtype=jnp.float32)
    blocks = 0.5 * identity[None, :, :] + 0.5 * jnp.einsum('bij,bkj->bik', random_part, random_part) / CENTRE_DEV
    return blocks.reshape(CENTRES, CENTRE_DEV).astype(jnp.bfloat16)


def steps_of(own_key, shape, shards, low, largest):
    def one(axis_at, parts):
        heights = jax.random.uniform(jax.random.fold_in(jax.random.fold_in(own_key, 6), axis_at), (parts,), jnp.float32, low / len(shards), largest / len(shards))
        return jnp.repeat(jnp.exp(heights), shape[axis_at] // parts).reshape((-1,) + (1,) * (len(shape) - axis_at - 1))

    level = one(*shards[0])
    for cut in shards[1:]:
        level = level * one(*cut)
    return level


def normal_values(rng, dims, deviation, most, split=(), kind=jnp.bfloat16):
    level = steps_of(rng, dims, split, -0.22, 0.18) if split else 1.0
    values = jax.random.normal(rng, dims, jnp.float32) * deviation * level
    return jnp.minimum(jnp.maximum(values, -most), most).astype(kind)


def setup_inputs(seed: int = 0) -> dict:
    arg_keys = jax.random.split(jax.random.key(seed), 5)
    return {
        "features": draw_features(jax.random.fold_in(arg_keys[4], 71), 0),
        "targets": normal_values(arg_keys[1], (ROWS_ALL, TARGETS), 1.0, 6.0, ((0, 16),)),
        "centre_points": draw_centre_points(jax.random.fold_in(arg_keys[4], 71), 0),
        "precond": draw_precond(jax.random.fold_in(arg_keys[4], 71), 0),
    }


RIDGE_WEIGHT = 0.02

def reference(features, targets, centre_points, precond):
    row_total = features.shape[0]
    feature_float = features.astype(jnp.float32)
    row_scale = 1.0 / jnp.sqrt(lax.optimization_barrier(jnp.mean(feature_float * feature_float, axis=1)) + 1e-06)
    centre_blocks = centre_points.reshape(N_CENTRES, CENTRE_DEV, D)
    group_rows = jnp.float32(ROW_DEV)

    def build(centre_block):
        inner_products = jnp.dot(features, centre_block.T, preferred_element_type=jnp.float32)
        centre_float = centre_block.astype(jnp.float32)
        centre_scale = 1.0 / jnp.sqrt(lax.optimization_barrier(jnp.mean(centre_float * centre_float, axis=1)) + 1e-06)
        cosine = inner_products * row_scale[:, None] * centre_scale[None, :] / jnp.float32(D)
        return jnp.exp(8.0 * (cosine - 1.0)).astype(jnp.bfloat16)
    kernel = lax.map(build, centre_blocks)

    def apply_rows(direction):
        narrow = direction.astype(jnp.bfloat16).reshape(N_CENTRES, CENTRE_DEV, TARGETS)

        def accumulate(running, pair):
            kernel_block, piece = pair
            return (running + jnp.dot(kernel_block, piece, preferred_element_type=jnp.float32), None)
        start_value = jnp.zeros((row_total, TARGETS), jnp.float32)
        result, unused_out = lax.scan(accumulate, start_value, (kernel, narrow))
        return result

    def apply_columns(rounded, divisor):

        def column_block(kernel_block):
            return jnp.dot(kernel_block.T, rounded, preferred_element_type=jnp.float32)
        return lax.map(column_block, kernel).reshape(N_CENTRES * CENTRE_DEV, TARGETS) / divisor
    precond_blocks = precond.reshape(N_CENTRES, CENTRE_DEV, CENTRE_DEV)

    def precondition(residual):
        narrow = residual.astype(jnp.bfloat16).reshape(N_CENTRES, CENTRE_DEV, TARGETS)

        def one_block(pair):
            return jnp.dot(pair[0], pair[1], preferred_element_type=jnp.float32)
        return lax.map(one_block, (precond_blocks, narrow)).reshape(N_CENTRES * CENTRE_DEV, TARGETS)
    rhs = apply_columns(targets, jnp.sqrt(group_rows))
    coefficients = jnp.zeros_like(rhs)
    fitted = jnp.zeros((row_total, TARGETS), jnp.float32)
    residual = rhs
    scaled = precondition(residual)
    direction = scaled
    product_now = lax.optimization_barrier(jnp.sum(residual * scaled, axis=0))
    for iteration in range(ITERS):
        applied_rows = apply_rows(direction)
        applied = apply_columns(applied_rows.astype(jnp.bfloat16), group_rows) + RIDGE_WEIGHT * direction
        step_size = product_now / lax.optimization_barrier(jnp.sum(direction * applied, axis=0))
        coefficients = coefficients + step_size * direction
        fitted = fitted + step_size * applied_rows
        residual = residual - step_size * applied
        if iteration + 1 < ITERS:
            scaled = precondition(residual)
            product_next = lax.optimization_barrier(jnp.sum(residual * scaled, axis=0))
            direction = scaled + product_next / product_now * direction
            product_now = product_next
    return (coefficients, fitted)
```

```python
import jax
import jax.numpy as jnp
from jax import lax
from jax.sharding import PartitionSpec as P

RIDGE_WEIGHT = 0.02


def exchanged(tiles, axis):
    return lax.all_to_all(tiles, axis, split_axis=0, concat_axis=0, tiled=True)


def copies_of(value, axis):
    copies = jnp.broadcast_to(value, (lax.axis_size(axis), *value.shape))
    return exchanged(copies, axis)


def two_halves(rows):
    high = rows.astype(jnp.bfloat16)
    low = (rows - high.astype(jnp.float32)).astype(jnp.bfloat16)
    return high, low


def extra_rows(sums):
    parts = [p[None, :] for s in sums for p in two_halves(s)]
    width = sums[0].shape[0]
    parts.append(jnp.zeros((8 - len(parts), width), jnp.bfloat16))
    return jnp.concatenate(parts, axis=0)


def summed_shares(partial, sums, axis):
    size = lax.axis_size(axis)
    share = partial.shape[0] // size
    tiles = partial.astype(jnp.bfloat16).reshape(size, share, partial.shape[1])
    if sums:
        rows = extra_rows(sums)
        tiles = jnp.concatenate(
            [tiles, jnp.broadcast_to(rows, (size, *rows.shape))], axis=1
        )
    arrived = exchanged(tiles, axis).astype(jnp.float32).sum(axis=0)
    totals = [arrived[share + 2 * i] + arrived[share + 2 * i + 1] for i in range(len(sums))]
    return arrived[:share], totals


def per_device(features, targets, centre_points, precond):
    group_rows = float(features.shape[0])
    gathered = copies_of(features.T, "centres").reshape(-1, features.shape[0])
    feature_count = gathered.shape[0]
    gathered_float = gathered.astype(jnp.float32)
    centre_float = centre_points.astype(jnp.float32)
    row_scale = 1.0 / jnp.sqrt(jnp.mean(gathered_float * gathered_float, axis=0) + 1e-06)
    centre_scale = 1.0 / jnp.sqrt(jnp.mean(centre_float * centre_float, axis=1) + 1e-06)
    inner_products = jnp.dot(centre_points, gathered, preferred_element_type=jnp.float32)
    cosine = (
        inner_products * row_scale[None, :] * centre_scale[:, None] / jnp.float32(feature_count)
    )
    kernel = jnp.exp(8.0 * (cosine - 1.0)).astype(jnp.bfloat16)

    def transposed(values):
        return jnp.dot(kernel, values, preferred_element_type=jnp.float32)

    def forward(values):
        return jnp.einsum(
            "cr,ct->rt", kernel, values.astype(jnp.bfloat16), preferred_element_type=jnp.float32
        )

    def precondition(residual):
        return jnp.dot(precond, residual, preferred_element_type=jnp.float32)

    def whole(share, axis):
        return copies_of(share.astype(jnp.bfloat16), axis).reshape(-1, share.shape[1])

    def column_sum(a, b):
        return jnp.sum(a * b, axis=0)

    position = lax.axis_index("rows")
    residual_share, _ = summed_shares(
        transposed(targets) / jnp.sqrt(jnp.float32(group_rows)), [], "rows"
    )
    residual = whole(residual_share, "rows")
    direction = precondition(residual)
    sums = [
        column_sum(residual.astype(jnp.float32), direction),
        column_sum(direction, direction),
    ]
    rows_share, (product_now, direction_sq) = summed_shares(forward(direction), sums, "centres")
    rounded = whole(rows_share, "centres")
    rounded_float = rounded.astype(jnp.float32)
    column_share, (rows_sq,) = summed_shares(
        transposed(rounded) / group_rows, [column_sum(rounded_float, rounded_float)], "rows"
    )
    share = column_share.shape[0]
    direction_share = lax.dynamic_slice_in_dim(direction, position * share, share, 0)
    step_size = product_now / (rows_sq / group_rows + RIDGE_WEIGHT * direction_sq)
    residual_share = residual_share - step_size * (column_share + RIDGE_WEIGHT * direction_share)
    residual = whole(residual_share, "rows")
    scaled = precondition(residual)
    sums = [
        column_sum(residual.astype(jnp.float32), scaled),
        column_sum(scaled, scaled),
        column_sum(scaled, direction),
    ]
    scaled_rows_share, (product_next, scaled_sq, cross_term) = summed_shares(
        forward(scaled), sums, "centres"
    )
    momentum = product_next / product_now
    next_sq = scaled_sq + 2.0 * momentum * cross_term + momentum * momentum * direction_sq
    next_direction = scaled + momentum * direction
    next_rows_share = scaled_rows_share + momentum * rows_share
    next_rows = whole(next_rows_share, "centres").astype(jnp.float32)
    rows_sq = jnp.sum(copies_of(column_sum(next_rows, next_rows)[None], "rows"), axis=(0, 1))
    next_step = product_next / (rows_sq / group_rows + RIDGE_WEIGHT * next_sq)
    coefficients = step_size * direction + next_step * next_direction
    fitted = step_size * rounded_float + next_step * next_rows
    return (coefficients, fitted)


def solution(mesh):
    return jax.shard_map(
        per_device,
        mesh=mesh,
        in_specs=(P("rows", "centres"), P("rows", None), P("centres", None), P("centres", None)),
        out_specs=(P("centres", None), P("rows", None)),
        check_vma=False,
    )
```

```python
import jax
import jax.numpy as jnp
from jax import lax
from jax.sharding import Mesh, PartitionSpec as P

RIDGE_WEIGHT = 0.02


def exchanged(tiles, axis):
    return lax.all_to_all(tiles, axis, split_axis=0, concat_axis=0, tiled=True)


def copies_of(value, axis):
    copies = jnp.broadcast_to(value, (lax.axis_size(axis), *value.shape))
    return exchanged(copies, axis)


def two_halves(rows):
    high = rows.astype(jnp.bfloat16)
    low = (rows - high.astype(jnp.float32)).astype(jnp.bfloat16)
    return high, low


def extra_rows(sums):
    parts = [p[None, :] for s in sums for p in two_halves(s)]
    return jnp.concatenate((parts * 4)[:8], axis=0)


def with_sums(tiles, sums):
    if not sums:
        return tiles
    rows = extra_rows(sums)
    return jnp.concatenate(
        [tiles, jnp.broadcast_to(rows, (tiles.shape[0], *rows.shape))], axis=1
    )


def totalled(arrived, share, count):
    total = arrived.astype(jnp.float32).sum(axis=0)
    sums = [total[share + 2 * i] + total[share + 2 * i + 1] for i in range(count)]
    return total[:share], sums


def summed_shares(partial, sums, axis):
    size = lax.axis_size(axis)
    share = partial.shape[0] // size
    tiles = partial.astype(jnp.bfloat16).reshape(size, share, partial.shape[1])
    return totalled(exchanged(with_sums(tiles, sums), axis), share, len(sums))


def summed_directly(share, sums, axis):
    tiles = jnp.broadcast_to(share.astype(jnp.bfloat16), (lax.axis_size(axis), *share.shape))
    return totalled(exchanged(with_sums(tiles, sums), axis), share.shape[0], len(sums))


def summed_in_plane(partial, sums):
    share, sums = summed_shares(partial, sums, "y")
    return summed_directly(share, sums, "x")


def per_device(features, targets, centre_points, precond):
    group_rows = float(features.shape[0])
    gathered = copies_of(features.T, ("x", "y")).reshape(-1, features.shape[0])
    gathered, centre_points = lax.optimization_barrier((gathered, centre_points))
    feature_count = gathered.shape[0]
    gathered_float = gathered.astype(jnp.float32)
    centre_float = centre_points.astype(jnp.float32)
    row_scale = 1.0 / jnp.sqrt(jnp.mean(gathered_float * gathered_float, axis=0) + 1e-06)
    centre_scale = 1.0 / jnp.sqrt(jnp.mean(centre_float * centre_float, axis=1) + 1e-06)
    inner_products = jnp.dot(centre_points, gathered, preferred_element_type=jnp.float32)
    cosine = (
        inner_products * row_scale[None, :] * centre_scale[:, None] / jnp.float32(feature_count)
    )
    kernel = jnp.exp(8.0 * (cosine - 1.0)).astype(jnp.bfloat16)

    def transposed(values):
        return jnp.dot(kernel, values, preferred_element_type=jnp.float32)

    def forward(values):
        return jnp.einsum(
            "cr,ct->rt", kernel, values.astype(jnp.bfloat16), preferred_element_type=jnp.float32
        )

    def precondition(residual):
        return jnp.dot(precond, residual, preferred_element_type=jnp.float32)

    def whole(share, axis):
        return copies_of(share.astype(jnp.bfloat16), axis).reshape(-1, share.shape[1])

    def column_sum(a, b):
        return jnp.sum(a * b, axis=0)

    residual_share, _ = summed_shares(
        transposed(targets) / jnp.sqrt(jnp.float32(group_rows)), [], "rows"
    )
    residual = whole(residual_share, "rows")
    direction = precondition(residual)
    sums = [
        column_sum(residual.astype(jnp.float32), direction),
        column_sum(direction, direction),
    ]
    rows_share, (product_now, direction_sq) = summed_in_plane(forward(direction), sums)
    rounded = whole(rows_share, "y")
    rounded_float = rounded.astype(jnp.float32)
    ridge_part = (RIDGE_WEIGHT / lax.axis_size("rows")) * direction
    applied_share, (rows_sq,) = summed_shares(
        transposed(rounded) / group_rows + ridge_part, [column_sum(rounded_float, rounded_float)], "rows"
    )
    step_size = product_now / (rows_sq / group_rows + RIDGE_WEIGHT * direction_sq)
    residual_share = residual_share - step_size * applied_share
    residual = whole(residual_share, "rows")
    scaled = precondition(residual)
    sums = [
        column_sum(residual.astype(jnp.float32), scaled),
        column_sum(scaled, scaled),
        column_sum(scaled, direction),
    ]
    scaled_rows_share, (product_next, scaled_sq, cross_term) = summed_in_plane(
        forward(scaled), sums
    )
    momentum = product_next / product_now
    next_sq = scaled_sq + 2.0 * momentum * cross_term + momentum * momentum * direction_sq
    next_direction = scaled + momentum * direction
    next_rows_share = scaled_rows_share + momentum * rows_share
    next_rows = whole(next_rows_share, "y").astype(jnp.float32)
    rows_sq = jnp.sum(copies_of(column_sum(next_rows, next_rows)[None], "rows"), axis=(0, 1))
    next_step = product_next / (rows_sq / group_rows + RIDGE_WEIGHT * next_sq)
    coefficients = step_size * direction + next_step * next_direction
    fitted = step_size * rounded_float + next_step * next_rows
    return (coefficients, fitted)


def solution(mesh):
    rows, centres = mesh.devices.shape
    split = Mesh(mesh.devices.reshape(rows, centres // 8, 8), ("rows", "x", "y"))
    plane = ("x", "y")
    return jax.shard_map(
        per_device,
        mesh=split,
        in_specs=(P("rows", plane), P("rows", None), P(plane, None), P(plane, None)),
        out_specs=(P(plane, None), P("rows", None)),
        check_vma=False,
    )
```

```python
import jax
import jax.numpy as jnp
from jax import lax
from jax.sharding import Mesh, PartitionSpec as P

RIDGE_WEIGHT = 0.02


def exchanged(tiles, axis):
    return lax.all_to_all(tiles, axis, split_axis=0, concat_axis=0, tiled=True)


def copies_of(value, axis):
    copies = jnp.broadcast_to(value, (lax.axis_size(axis), *value.shape))
    return exchanged(copies, axis)


def two_halves(rows):
    high = rows.astype(jnp.bfloat16)
    low = (rows - high.astype(jnp.float32)).astype(jnp.bfloat16)
    return high, low


def extra_rows(sums):
    parts = [p[None, :] for s in sums for p in two_halves(s)]
    return jnp.concatenate((parts * 4)[:8], axis=0)


def with_sums(tiles, sums):
    if not sums:
        return tiles
    rows = extra_rows(sums)
    return jnp.concatenate(
        [tiles, jnp.broadcast_to(rows, (tiles.shape[0], *rows.shape))], axis=1
    )


def totalled(arrived, share, count):
    total = arrived.astype(jnp.float32).sum(axis=0)
    sums = [total[share + 2 * i] + total[share + 2 * i + 1] for i in range(count)]
    return total[:share], sums


def summed_shares(partial, sums, axis):
    size = lax.axis_size(axis)
    share = partial.shape[0] // size
    tiles = partial.astype(jnp.bfloat16).reshape(size, share, partial.shape[1])
    return totalled(exchanged(with_sums(tiles, sums), axis), share, len(sums))


def summed_directly(share, sums, axis):
    tiles = jnp.broadcast_to(share.astype(jnp.bfloat16), (lax.axis_size(axis), *share.shape))
    return totalled(exchanged(with_sums(tiles, sums), axis), share.shape[0], len(sums))


def summed_in_plane(partial, sums):
    return summed_shares(partial, sums, ("x", "y"))


def per_device(features, targets, centre_points, precond):
    group_rows = float(features.shape[0])
    group_parts = copies_of(features.T, "y")
    gathered = copies_of(group_parts, "x").reshape(-1, features.shape[0])
    gathered, centre_points = lax.optimization_barrier((gathered, centre_points))
    feature_count = gathered.shape[0]
    gathered_float = gathered.astype(jnp.float32)
    centre_float = centre_points.astype(jnp.float32)
    row_scale = 1.0 / jnp.sqrt(jnp.mean(gathered_float * gathered_float, axis=0) + 1e-06)
    centre_scale = 1.0 / jnp.sqrt(jnp.mean(centre_float * centre_float, axis=1) + 1e-06)
    inner_products = jnp.dot(centre_points, gathered, preferred_element_type=jnp.float32)
    cosine = (
        inner_products * row_scale[None, :] * centre_scale[:, None] / jnp.float32(feature_count)
    )
    kernel = jnp.exp(8.0 * (cosine - 1.0)).astype(jnp.bfloat16)

    def transposed(values):
        return jnp.dot(kernel, values, preferred_element_type=jnp.float32)

    def forward(values):
        return jnp.einsum(
            "cr,ct->rt", kernel, values.astype(jnp.bfloat16), preferred_element_type=jnp.float32
        )

    def precondition(residual):
        return jnp.dot(precond, residual, preferred_element_type=jnp.float32)

    def whole(share, axis):
        return copies_of(share.astype(jnp.bfloat16), axis).reshape(-1, share.shape[1])

    def column_sum(a, b):
        return jnp.sum(a * b, axis=0)

    residual_share, _ = summed_shares(
        transposed(targets) / jnp.sqrt(jnp.float32(group_rows)), [], "rows"
    )
    residual = whole(residual_share, "rows")
    direction = precondition(residual)
    sums = [
        column_sum(residual.astype(jnp.float32), direction),
        column_sum(direction, direction),
    ]
    rows_share, (product_now, direction_sq) = summed_in_plane(forward(direction), sums)
    rounded = whole(rows_share, ("x", "y"))
    rounded_float = rounded.astype(jnp.float32)
    ridge_part = (RIDGE_WEIGHT / lax.axis_size("rows")) * direction
    applied_share, (rows_sq,) = summed_shares(
        transposed(rounded) / group_rows + ridge_part, [column_sum(rounded_float, rounded_float)], "rows"
    )
    step_size = product_now / (rows_sq / group_rows + RIDGE_WEIGHT * direction_sq)
    residual_share = residual_share - step_size * applied_share
    residual = whole(residual_share, "rows")
    scaled = precondition(residual)
    sums = [
        column_sum(residual.astype(jnp.float32), scaled),
        column_sum(scaled, scaled),
        column_sum(scaled, direction),
    ]
    scaled_rows_share, (product_next, scaled_sq, cross_term) = summed_in_plane(
        forward(scaled), sums
    )
    momentum = product_next / product_now
    next_sq = scaled_sq + 2.0 * momentum * cross_term + momentum * momentum * direction_sq
    next_direction = scaled + momentum * direction
    next_rows_share = scaled_rows_share + momentum * rows_share
    next_rows = whole(next_rows_share, ("x", "y")).astype(jnp.float32)
    rows_sq = jnp.sum(copies_of(column_sum(next_rows, next_rows)[None], "rows"), axis=(0, 1))
    next_step = product_next / (rows_sq / group_rows + RIDGE_WEIGHT * next_sq)
    coefficients = step_size * direction + next_step * next_direction
    fitted = step_size * rounded_float + next_step * next_rows
    return (coefficients, fitted)


def solution(mesh):
    rows, centres = mesh.devices.shape
    split = Mesh(mesh.devices.reshape(rows, centres // 8, 8), ("rows", "x", "y"))
    plane = ("x", "y")
    return jax.shard_map(
        per_device,
        mesh=split,
        in_specs=(P("rows", plane), P("rows", None), P(plane, None), P(plane, None)),
        out_specs=(P(plane, None), P("rows", None)),
        check_vma=False,
    )
```

```python
import jax
import jax.numpy as jnp
from jax import lax
from jax.experimental.layout import Layout, with_layout_constraint
from jax.sharding import Mesh, PartitionSpec as P

RIDGE_WEIGHT = 0.02


def exchanged(tiles, axis):
    return lax.all_to_all(tiles, axis, split_axis=0, concat_axis=0, tiled=True)


def copies_of(value, axis):
    copies = jnp.broadcast_to(value, (lax.axis_size(axis), *value.shape))
    return exchanged(copies, axis)


def summed_shares(partial, sums, axis):
    size = lax.axis_size(axis)
    width = partial.shape[1]
    if not sums:
        tiles = partial.astype(jnp.bfloat16).reshape(size, -1, width)
        return exchanged(tiles, axis).astype(jnp.float32).sum(axis=0), []
    pairs = partial.shape[0] // size // 2
    tiles = partial.astype(jnp.bfloat16).reshape(size, pairs, 2, width)
    rows = list(sums) + [sums[0]] * (len(sums) % 2)
    rows = jnp.stack(rows).astype(jnp.bfloat16).reshape(1, -1, 2, width)
    tiles = jnp.concatenate([tiles, jnp.broadcast_to(rows, (size, *rows.shape[1:]))], axis=1)
    total = exchanged(tiles, axis).astype(jnp.float32).sum(axis=0)
    totals = [total[pairs + i // 2, i % 2] for i in range(len(sums))]
    return total[:pairs].reshape(-1, width), totals


def summed_in_plane(partial, sums):
    return summed_shares(partial, sums, ("x", "y"))


def per_device(features, targets, centre_points, precond):
    group_rows = float(features.shape[0])
    group_parts = copies_of(features.T, "y")
    gathered = copies_of(group_parts, "x").reshape(-1, features.shape[0])
    gathered, centre_points = lax.optimization_barrier((gathered, centre_points))
    feature_count = gathered.shape[0]
    gathered_float = gathered.astype(jnp.float32)
    centre_float = centre_points.astype(jnp.float32)
    row_scale = 1.0 / jnp.sqrt(jnp.mean(gathered_float * gathered_float, axis=0) + 1e-06)
    centre_scale = 1.0 / jnp.sqrt(jnp.mean(centre_float * centre_float, axis=1) + 1e-06)
    inner_products = jnp.dot(centre_points, gathered, preferred_element_type=jnp.float32)
    cosine = (
        inner_products * row_scale[None, :] * centre_scale[:, None] / jnp.float32(feature_count)
    )
    kernel = jnp.exp(8.0 * (cosine - 1.0)).astype(jnp.bfloat16)

    def transposed(values):
        return jnp.dot(kernel, values, preferred_element_type=jnp.float32)

    def forward(values):
        return jnp.einsum(
            "cr,ct->rt", kernel, values.astype(jnp.bfloat16), preferred_element_type=jnp.float32
        )

    def precondition(residual):
        product = jnp.dot(precond, residual, preferred_element_type=jnp.float32)
        return with_layout_constraint(product, Layout((0, 1)))

    def whole(share, axis):
        return copies_of(share.astype(jnp.bfloat16), axis).reshape(-1, share.shape[1])

    def column_sum(a, b):
        return jnp.sum(a * b, axis=0)

    residual_share, _ = summed_shares(
        transposed(targets) / jnp.sqrt(jnp.float32(group_rows)), [], "rows"
    )
    residual = whole(residual_share, "rows")
    direction = precondition(residual)
    sums = [
        column_sum(residual.astype(jnp.float32), direction),
        column_sum(direction, direction),
    ]
    rows_share, (product_now, direction_sq) = summed_in_plane(forward(direction), sums)
    rounded = whole(rows_share, ("x", "y"))
    rounded_float = rounded.astype(jnp.float32)
    ridge_part = (RIDGE_WEIGHT / lax.axis_size("rows")) * direction
    applied_share, (rows_sq,) = summed_shares(
        transposed(rounded) / group_rows + ridge_part, [column_sum(rounded_float, rounded_float)], "rows"
    )
    step_size = product_now / (rows_sq / group_rows + RIDGE_WEIGHT * direction_sq)
    residual_share = residual_share - step_size * applied_share
    residual = whole(residual_share, "rows")
    scaled = precondition(residual)
    sums = [
        column_sum(residual.astype(jnp.float32), scaled),
        column_sum(scaled, scaled),
        column_sum(scaled, direction),
    ]
    scaled_rows_share, (product_next, scaled_sq, cross_term) = summed_in_plane(
        forward(scaled), sums
    )
    momentum = product_next / product_now
    next_sq = scaled_sq + 2.0 * momentum * cross_term + momentum * momentum * direction_sq
    next_direction = scaled + momentum * direction
    next_rows_share = scaled_rows_share + momentum * rows_share
    next_rows = whole(next_rows_share, ("x", "y")).astype(jnp.float32)
    rows_sq = jnp.sum(copies_of(column_sum(next_rows, next_rows)[None], "rows"), axis=(0, 1))
    next_step = product_next / (rows_sq / group_rows + RIDGE_WEIGHT * next_sq)
    coefficients = step_size * direction + next_step * next_direction
    fitted = step_size * rounded_float + next_step * next_rows
    return (coefficients, fitted)


def solution(mesh):
    rows, centres = mesh.devices.shape
    split = Mesh(mesh.devices.reshape(rows, centres // 8, 8), ("rows", "x", "y"))
    plane = ("x", "y")
    return jax.shard_map(
        per_device,
        mesh=split,
        in_specs=(P("rows", plane), P("rows", None), P(plane, None), P(plane, None)),
        out_specs=(P(plane, None), P("rows", None)),
        check_vma=False,
    )
```

```python
import jax
import jax.numpy as jnp
from jax import lax
from jax.experimental import pallas as pl
from jax.experimental.pallas import tpu as pltpu
from jax.sharding import Mesh, PartitionSpec as P

RIDGE_WEIGHT = 0.02


def exchanged(tiles, axis):
    return lax.all_to_all(tiles, axis, split_axis=0, concat_axis=0, tiled=True)


def copies_of(value, axis):
    copies = jnp.broadcast_to(value, (lax.axis_size(axis), *value.shape))
    return exchanged(copies, axis)


def per_device(features, targets, centre_points, precond):
    group_rows = float(features.shape[0])
    group_parts = copies_of(features.T, "y")
    gathered = copies_of(group_parts, "x").reshape(-1, features.shape[0])
    gathered, centre_points = lax.optimization_barrier((gathered, centre_points))
    kernel, product = built(centre_points, gathered, targets, group_rows)

    def whole(share, axis):
        return copies_of(share.astype(jnp.bfloat16), axis).reshape(-1, share.shape[1])

    def column_sum(a, b):
        return jnp.sum(a * b, axis=0)

    tiles = product.reshape(lax.axis_size("rows"), -1, product.shape[1])
    residual_share = exchanged(tiles, "rows").astype(jnp.float32).sum(axis=0)
    residual = whole(residual_share, "rows")
    share = features.shape[0] // lax.axis_size(("x", "y"))
    direction, rows_share, (product_now, direction_sq) = stepped(
        precond, residual, kernel, None, share
    )
    rounded = whole(rows_share, ("x", "y"))
    applied_share, rows_sq = returned(kernel, rounded, direction, group_rows, "rows")
    step_size = product_now / (rows_sq / group_rows + RIDGE_WEIGHT * direction_sq)
    residual_share = residual_share - step_size * applied_share
    residual = whole(residual_share, "rows")
    scaled, scaled_rows_share, (product_next, scaled_sq, cross_term) = stepped(
        precond, residual, kernel, direction, share
    )
    momentum = product_next / product_now
    next_sq = scaled_sq + 2.0 * momentum * cross_term + momentum * momentum * direction_sq
    next_rows_share = scaled_rows_share + momentum * rows_share
    known = jnp.stack([step_size, momentum, product_next, next_sq])
    next_rows_share, known = lax.optimization_barrier((next_rows_share, known))
    next_rows = whole(next_rows_share, ("x", "y"))
    next_parts = column_sum(next_rows.astype(jnp.float32), next_rows.astype(jnp.float32))
    row_parts = copies_of(next_parts[None], "rows").reshape(-1, next_parts.shape[-1])
    return finished(row_parts, known, direction, scaled, rounded, next_rows, group_rows)


FAST = pl.BlockSpec(memory_space=pltpu.VMEM)


def built(centre_points, gathered, targets, group_rows):
    feature_count, rows = gathered.shape
    centres = centre_points.shape[0]
    band = centres // 4

    def body(centre_points, gathered, targets, kernel, product):
        gathered_float = gathered[...].astype(jnp.float32)
        squares = jnp.sum(gathered_float * gathered_float, axis=0, keepdims=True)
        row_scale = 1.0 / jnp.sqrt(squares / feature_count + 1e-06)
        for at in range(0, centres, band):
            points = centre_points[at : at + band, :]
            point_float = points.astype(jnp.float32)
            squares = jnp.sum(point_float * point_float, axis=1, keepdims=True)
            centre_scale = 1.0 / jnp.sqrt(squares / feature_count + 1e-06)
            inner = jnp.dot(points, gathered[...], preferred_element_type=jnp.float32)
            cosine = inner * row_scale * centre_scale / feature_count
            values = jnp.exp(8.0 * (cosine - 1.0)).astype(jnp.bfloat16)
            kernel[at : at + band, :] = values
            part = jnp.dot(values, targets[...], preferred_element_type=jnp.float32)
            product[at : at + band, :] = (part / group_rows**0.5).astype(jnp.bfloat16)

    return pl.pallas_call(
        body,
        out_shape=[
            jax.ShapeDtypeStruct((centres, rows), jnp.bfloat16),
            jax.ShapeDtypeStruct((centres, targets.shape[1]), jnp.bfloat16),
        ],
        in_specs=[FAST] * 3,
        out_specs=[FAST] * 2,
        compiler_params=pltpu.CompilerParams(vmem_limit_bytes=12 * 2**20),
        name="built",
    )(centre_points, gathered, targets)


def returned(kernel, rounded, direction, group_rows, axis):
    size = lax.axis_size(axis)
    centres, width = direction.shape
    share = centres // size
    whole_share = share + 2
    part = RIDGE_WEIGHT / size

    def body(kernel, rounded, direction, packed):
        held = rounded[...]
        held_float = held.astype(jnp.float32)
        squares = jnp.sum(held_float * held_float, axis=0, keepdims=True)
        tail = jnp.concatenate([squares, squares], axis=0).astype(jnp.bfloat16)
        product = jnp.dot(kernel[...], held, preferred_element_type=jnp.float32)
        product = (product / group_rows + part * direction[...]).astype(jnp.bfloat16)
        for k in range(size):
            at = k * whole_share
            packed[at : at + share, :] = product[k * share : (k + 1) * share, :]
            packed[at + share : at + whole_share, :] = tail

    packed = pl.pallas_call(
        body,
        out_shape=jax.ShapeDtypeStruct((size * whole_share, width), jnp.bfloat16),
        in_specs=[FAST] * 3,
        out_specs=FAST,
        compiler_params=pltpu.CompilerParams(vmem_limit_bytes=8 * 2**20),
        name="returned",
    )(kernel, rounded, direction)
    arrived = exchanged(packed.reshape(size, whole_share // 2, 2, width), axis)
    total = arrived.astype(jnp.float32).sum(axis=0)
    return total[: share // 2].reshape(-1, width), total[share // 2, 0]


def stepped(precond, residual, kernel, older, share):
    centres, rows = kernel.shape
    width = residual.shape[1]
    size = rows // share
    extra = 2 if older is None else 4
    whole_share = share + extra

    def body(precond, residual, kernel, *rest):
        (scaled_out, packed), olds = rest[-2:], rest[:-2]
        held = residual[...]
        scaled = jnp.dot(precond[...], held, preferred_element_type=jnp.float32)
        scaled_out[...] = scaled
        sums = [
            jnp.sum(held.astype(jnp.float32) * scaled, axis=0, keepdims=True),
            jnp.sum(scaled * scaled, axis=0, keepdims=True),
        ]
        for old in olds:
            sums.append(jnp.sum(scaled * old[...], axis=0, keepdims=True))
            sums.append(sums[0])
        tail = jnp.concatenate(sums, axis=0).astype(jnp.bfloat16)
        product = lax.dot_general(
            kernel[...],
            scaled.astype(jnp.bfloat16),
            (((0,), (0,)), ((), ())),
            preferred_element_type=jnp.float32,
        ).astype(jnp.bfloat16)
        for k in range(size):
            at = k * whole_share
            packed[at : at + share, :] = product[k * share : (k + 1) * share, :]
            packed[at + share : at + whole_share, :] = tail

    operands = [precond, residual, kernel] + ([] if older is None else [older])
    scaled, packed = pl.pallas_call(
        body,
        out_shape=[
            jax.ShapeDtypeStruct((centres, width), jnp.float32),
            jax.ShapeDtypeStruct((size * whole_share, width), jnp.bfloat16),
        ],
        in_specs=[FAST] * len(operands),
        out_specs=[FAST] * 2,
        compiler_params=pltpu.CompilerParams(vmem_limit_bytes=8 * 2**20),
        name="stepped",
    )(*operands)
    arrived = exchanged(packed.reshape(size, whole_share // 2, 2, width), ("x", "y"))
    total = arrived.astype(jnp.float32).sum(axis=0)
    sums = [total[share // 2 + i // 2, i % 2] for i in range(2 if older is None else 3)]
    return scaled, total[: share // 2].reshape(-1, width), sums


def finished(row_parts, known, direction, scaled, rows, next_rows, group_rows):

    def body(parts, known, direction, scaled, rows, next_rows, *rest):
        outputs, held, done = rest[:2], rest[2:4], rest[4]
        rows_sq = jnp.sum(parts[...], axis=0, keepdims=True)
        step_size, momentum = known[0:1, :], known[1:2, :]
        next_step = known[2:3, :] / (rows_sq / group_rows + RIDGE_WEIGHT * known[3:4, :])
        copies = [
            pltpu.make_async_copy(held[i], outputs[i], done.at[i]) for i in range(2)
        ]
        both = rows[...].astype(jnp.float32), next_rows[...].astype(jnp.float32)
        held[1][...] = step_size * both[0] + next_step * both[1]
        copies[1].start()
        old = direction[...]
        held[0][...] = step_size * old + next_step * (scaled[...] + momentum * old)
        copies[0].start()
        copies[1].wait()
        copies[0].wait()

    shapes = [
        jax.ShapeDtypeStruct(direction.shape, jnp.float32),
        jax.ShapeDtypeStruct(rows.shape, jnp.float32),
    ]
    return tuple(
        pl.pallas_call(
            body,
            out_shape=shapes,
            in_specs=[FAST] * 6,
            out_specs=[pl.BlockSpec(memory_space=pl.ANY)] * 2,
            scratch_shapes=[pltpu.VMEM(x.shape, x.dtype) for x in shapes]
            + [pltpu.SemaphoreType.DMA((2,))],
            compiler_params=pltpu.CompilerParams(vmem_limit_bytes=4 * 2**20),
            name="finished",
        )(row_parts, known, direction, scaled, rows, next_rows)
    )


def solution(mesh):
    rows, centres = mesh.devices.shape
    split = Mesh(mesh.devices.reshape(rows, centres // 8, 8), ("rows", "x", "y"))
    plane = ("x", "y")
    return jax.shard_map(
        per_device,
        mesh=split,
        in_specs=(P("rows", plane), P("rows", None), P(plane, None), P(plane, None)),
        out_specs=(P(plane, None), P("rows", None)),
        check_vma=False,
    )
```

```python
import jax
import jax.numpy as jnp
from jax import lax
from jax.experimental import pallas as pl
from jax.experimental.pallas import tpu as pltpu
from jax.sharding import Mesh, PartitionSpec as P

RIDGE_WEIGHT = 0.02
ROWS = ("core", "z")


def exchanged(tiles, axis):
    return lax.all_to_all(tiles, axis, split_axis=0, concat_axis=0, tiled=True)


def copies_of(value, axis):
    copies = jnp.broadcast_to(value, (lax.axis_size(axis), *value.shape))
    return exchanged(copies, axis)


def per_device(features, targets, centre_points, precond):
    group_rows = float(features.shape[0])
    group_parts = copies_of(features.T, "y")
    gathered = copies_of(group_parts, "x").reshape(-1, features.shape[0])
    gathered, centre_points = lax.optimization_barrier((gathered, centre_points))
    kernel, product = built(centre_points, gathered, targets, group_rows)

    def whole(share, axis):
        return copies_of(share.astype(jnp.bfloat16), axis).reshape(-1, share.shape[1])

    def column_sum(a, b):
        return jnp.sum(a * b, axis=0)

    tiles = product.reshape(lax.axis_size(ROWS), -1, product.shape[1])
    residual_share = exchanged(tiles, ROWS).astype(jnp.float32).sum(axis=0)
    residual = whole(residual_share, ROWS)
    share = features.shape[0] // lax.axis_size(("x", "y"))
    direction, rows_share, (product_now, direction_sq) = stepped(
        precond, residual, kernel, None, share
    )
    rounded = whole(rows_share, ("y", "x"))
    applied_share, rows_sq = returned(kernel, rounded, direction, group_rows, ROWS)
    step_size = product_now / (rows_sq / group_rows + RIDGE_WEIGHT * direction_sq)
    residual_share = residual_share - step_size * applied_share
    residual = whole(residual_share, ROWS)
    scaled, scaled_rows_share, (product_next, scaled_sq, cross_term) = stepped(
        precond, residual, kernel, direction, share
    )
    momentum = product_next / product_now
    next_sq = scaled_sq + 2.0 * momentum * cross_term + momentum * momentum * direction_sq
    next_rows_share = scaled_rows_share + momentum * rows_share
    known = jnp.stack([step_size, momentum, product_next, next_sq])
    next_rows_share, known = lax.optimization_barrier((next_rows_share, known))
    next_rows = whole(next_rows_share, ("y", "x"))
    next_parts = column_sum(next_rows.astype(jnp.float32), next_rows.astype(jnp.float32))
    row_parts = copies_of(next_parts[None], ROWS).reshape(-1, next_parts.shape[-1])
    return finished(row_parts, known, direction, scaled, rounded, next_rows, group_rows)


FAST = pl.BlockSpec(memory_space=pltpu.VMEM)


def built(centre_points, gathered, targets, group_rows):
    feature_count, rows = gathered.shape
    centres = centre_points.shape[0]
    band = centres // 4

    def body(centre_points, gathered, targets, kernel, product):
        gathered_float = gathered[...].astype(jnp.float32)
        squares = jnp.sum(gathered_float * gathered_float, axis=0, keepdims=True)
        row_scale = 1.0 / jnp.sqrt(squares / feature_count + 1e-06)
        for at in range(0, centres, band):
            points = centre_points[at : at + band, :]
            point_float = points.astype(jnp.float32)
            squares = jnp.sum(point_float * point_float, axis=1, keepdims=True)
            centre_scale = 1.0 / jnp.sqrt(squares / feature_count + 1e-06)
            inner = jnp.dot(points, gathered[...], preferred_element_type=jnp.float32)
            cosine = inner * row_scale * centre_scale / feature_count
            values = jnp.exp(8.0 * (cosine - 1.0)).astype(jnp.bfloat16)
            kernel[at : at + band, :] = values
            part = jnp.dot(values, targets[...], preferred_element_type=jnp.float32)
            product[at : at + band, :] = (part / group_rows**0.5).astype(jnp.bfloat16)

    return pl.pallas_call(
        body,
        out_shape=[
            jax.ShapeDtypeStruct((centres, rows), jnp.bfloat16),
            jax.ShapeDtypeStruct((centres, targets.shape[1]), jnp.bfloat16),
        ],
        in_specs=[FAST] * 3,
        out_specs=[FAST] * 2,
        compiler_params=pltpu.CompilerParams(vmem_limit_bytes=12 * 2**20),
        name="built",
    )(centre_points, gathered, targets)


def returned(kernel, rounded, direction, group_rows, axis):
    size = lax.axis_size(axis)
    centres, width = direction.shape
    share = centres // size
    whole_share = share + 2
    part = RIDGE_WEIGHT / size

    def body(kernel, rounded, direction, packed):
        held = rounded[...]
        held_float = held.astype(jnp.float32)
        squares = jnp.sum(held_float * held_float, axis=0, keepdims=True)
        tail = jnp.concatenate([squares, squares], axis=0).astype(jnp.bfloat16)
        product = jnp.dot(kernel[...], held, preferred_element_type=jnp.float32)
        product = (product / group_rows + part * direction[...]).astype(jnp.bfloat16)
        for k in range(size):
            at = k * whole_share
            packed[at : at + share, :] = product[k * share : (k + 1) * share, :]
            packed[at + share : at + whole_share, :] = tail

    packed = pl.pallas_call(
        body,
        out_shape=jax.ShapeDtypeStruct((size * whole_share, width), jnp.bfloat16),
        in_specs=[FAST] * 3,
        out_specs=FAST,
        compiler_params=pltpu.CompilerParams(vmem_limit_bytes=8 * 2**20),
        name="returned",
    )(kernel, rounded, direction)
    arrived = exchanged(packed.reshape(size, whole_share // 2, 2, width), axis)
    total = arrived.astype(jnp.float32).sum(axis=0)
    return total[: share // 2].reshape(-1, width), total[share // 2, 0]


def stepped(precond, residual, kernel, older, share):
    centres, rows = kernel.shape
    width = residual.shape[1]
    size = rows // share
    extra = 2 if older is None else 4
    whole_share = share + extra

    def body(precond, residual, kernel, *rest):
        (scaled_out, packed), olds = rest[-2:], rest[:-2]
        held = residual[...]
        scaled = jnp.dot(precond[...], held, preferred_element_type=jnp.float32)
        scaled_out[...] = scaled
        sums = [
            jnp.sum(held.astype(jnp.float32) * scaled, axis=0, keepdims=True),
            jnp.sum(scaled * scaled, axis=0, keepdims=True),
        ]
        for old in olds:
            sums.append(jnp.sum(scaled * old[...], axis=0, keepdims=True))
            sums.append(sums[0])
        tail = jnp.concatenate(sums, axis=0).astype(jnp.bfloat16)
        product = lax.dot_general(
            kernel[...],
            scaled.astype(jnp.bfloat16),
            (((0,), (0,)), ((), ())),
            preferred_element_type=jnp.float32,
        ).astype(jnp.bfloat16)
        for k in range(size):
            at = k * whole_share
            packed[at : at + share, :] = product[k * share : (k + 1) * share, :]
            packed[at + share : at + whole_share, :] = tail

    operands = [precond, residual, kernel] + ([] if older is None else [older])
    scaled, packed = pl.pallas_call(
        body,
        out_shape=[
            jax.ShapeDtypeStruct((centres, width), jnp.float32),
            jax.ShapeDtypeStruct((size * whole_share, width), jnp.bfloat16),
        ],
        in_specs=[FAST] * len(operands),
        out_specs=[FAST] * 2,
        compiler_params=pltpu.CompilerParams(vmem_limit_bytes=8 * 2**20),
        name="stepped",
    )(*operands)
    arrived = exchanged(packed.reshape(size, whole_share // 2, 2, width), ("y", "x"))
    total = arrived.astype(jnp.float32).sum(axis=0)
    sums = [total[share // 2 + i // 2, i % 2] for i in range(2 if older is None else 3)]
    return scaled, total[: share // 2].reshape(-1, width), sums


def finished(row_parts, known, direction, scaled, rows, next_rows, group_rows):

    def body(parts, known, direction, scaled, rows, next_rows, *rest):
        outputs, held, done = rest[:2], rest[2:4], rest[4]
        rows_sq = jnp.sum(parts[...], axis=0, keepdims=True)
        step_size, momentum = known[0:1, :], known[1:2, :]
        next_step = known[2:3, :] / (rows_sq / group_rows + RIDGE_WEIGHT * known[3:4, :])
        copies = [
            pltpu.make_async_copy(held[i], outputs[i], done.at[i]) for i in range(2)
        ]
        both = rows[...].astype(jnp.float32), next_rows[...].astype(jnp.float32)
        held[1][...] = step_size * both[0] + next_step * both[1]
        copies[1].start()
        old = direction[...]
        held[0][...] = step_size * old + next_step * (scaled[...] + momentum * old)
        copies[0].start()
        copies[1].wait()
        copies[0].wait()

    shapes = [
        jax.ShapeDtypeStruct(direction.shape, jnp.float32),
        jax.ShapeDtypeStruct(rows.shape, jnp.float32),
    ]
    return tuple(
        pl.pallas_call(
            body,
            out_shape=shapes,
            in_specs=[FAST] * 6,
            out_specs=[pl.BlockSpec(memory_space=pl.ANY)] * 2,
            scratch_shapes=[pltpu.VMEM(x.shape, x.dtype) for x in shapes]
            + [pltpu.SemaphoreType.DMA((2,))],
            compiler_params=pltpu.CompilerParams(vmem_limit_bytes=4 * 2**20),
            name="finished",
        )(row_parts, known, direction, scaled, rows, next_rows)
    )


def solution(mesh):
    rows, centres = mesh.devices.shape
    split = Mesh(mesh.devices.reshape(rows // 2, 2, centres // 8, 8), ("z", "core", "x", "y"))
    held = ("z", "core")
    plane = ("x", "y")
    return jax.shard_map(
        per_device,
        mesh=split,
        in_specs=(P(held, plane), P(held, None), P(plane, None), P(plane, None)),
        out_specs=(P(plane, None), P(held, None)),
        check_vma=False,
    )
```

```python
import math

import jax
import jax.numpy as jnp
from jax import lax
from jax.experimental import pallas as pl
from jax.experimental.pallas import tpu as pltpu
from jax.sharding import Mesh, PartitionSpec as P

RIDGE_WEIGHT = 0.02
SHARP = 8.0 * math.log2(math.e)
ROWS = ("core", "z")


def exchanged(tiles, axis):
    return lax.all_to_all(tiles, axis, split_axis=0, concat_axis=0, tiled=True)


def copies_of(value, axis):
    copies = jnp.broadcast_to(value, (lax.axis_size(axis), *value.shape))
    return exchanged(copies, axis)


def per_device(features, targets, centre_points, precond):
    group_rows = float(features.shape[0])
    group_parts = copies_of(features.T, "y")
    gathered = copies_of(group_parts, "x").reshape(-1, features.shape[0])
    gathered, centre_points = lax.optimization_barrier((gathered, centre_points))
    kernel, product = built(centre_points, gathered, targets, group_rows)

    def whole(share, axis):
        return copies_of(share.astype(jnp.bfloat16), axis).reshape(-1, share.shape[1])

    def column_sum(a, b):
        return jnp.sum(a * b, axis=0)

    tiles = product.reshape(lax.axis_size(ROWS), -1, product.shape[1])
    residual_share = exchanged(tiles, ROWS).astype(jnp.float32).sum(axis=0)
    residual = whole(residual_share, ROWS)
    share = features.shape[0] // lax.axis_size(("x", "y"))
    direction, rows_share, (product_now, direction_sq) = stepped(
        precond, residual, kernel, None, share
    )
    rounded = whole(rows_share, ("y", "x"))
    applied_share, rows_sq = returned(kernel, rounded, direction, group_rows, ROWS)
    step_size = product_now / (rows_sq / group_rows + RIDGE_WEIGHT * direction_sq)
    residual_share = residual_share - step_size * applied_share
    residual = whole(residual_share, ROWS)
    scaled, scaled_rows_share, (product_next, scaled_sq, cross_term) = stepped(
        precond, residual, kernel, direction, share
    )
    momentum = product_next / product_now
    next_sq = scaled_sq + 2.0 * momentum * cross_term + momentum * momentum * direction_sq
    next_rows_share = scaled_rows_share + momentum * rows_share
    known = jnp.stack([step_size, momentum, product_next, next_sq])
    next_rows_share, known = lax.optimization_barrier((next_rows_share, known))
    next_rows = whole(next_rows_share, ("y", "x"))
    next_parts = column_sum(next_rows.astype(jnp.float32), next_rows.astype(jnp.float32))
    row_parts = copies_of(next_parts[None], ROWS).reshape(-1, next_parts.shape[-1])
    return finished(row_parts, known, direction, scaled, rounded, next_rows, group_rows)


FAST = pl.BlockSpec(memory_space=pltpu.VMEM)


def built(centre_points, gathered, targets, group_rows):
    feature_count, rows = gathered.shape
    centres = centre_points.shape[0]
    band = centres // 2

    def body(centre_points, gathered, targets, kernel, product):
        gathered_float = gathered[...].astype(jnp.float32)
        squares = jnp.sum(gathered_float * gathered_float, axis=0, keepdims=True)
        row_scale = 1.0 / jnp.sqrt(squares / feature_count + 1e-06)
        for at in range(0, centres, band):
            points = centre_points[at : at + band, :]
            point_float = points.astype(jnp.float32)
            squares = jnp.sum(point_float * point_float, axis=1, keepdims=True)
            centre_scale = (SHARP / feature_count) / jnp.sqrt(squares / feature_count + 1e-06)
            inner = jnp.dot(points, gathered[...], preferred_element_type=jnp.float32)
            values = jnp.exp2(inner * row_scale * centre_scale - SHARP).astype(jnp.bfloat16)
            kernel[at : at + band, :] = values
            part = jnp.dot(values, targets[...], preferred_element_type=jnp.float32)
            product[at : at + band, :] = (part / group_rows**0.5).astype(jnp.bfloat16)

    return pl.pallas_call(
        body,
        out_shape=[
            jax.ShapeDtypeStruct((centres, rows), jnp.bfloat16),
            jax.ShapeDtypeStruct((centres, targets.shape[1]), jnp.bfloat16),
        ],
        in_specs=[FAST] * 3,
        out_specs=[FAST] * 2,
        compiler_params=pltpu.CompilerParams(vmem_limit_bytes=12 * 2**20),
        name="built",
    )(centre_points, gathered, targets)


def returned(kernel, rounded, direction, group_rows, axis):
    size = lax.axis_size(axis)
    centres, width = direction.shape
    share = centres // size
    whole_share = share + 2
    part = RIDGE_WEIGHT / size

    def body(kernel, rounded, direction, packed):
        held = rounded[...]
        held_float = held.astype(jnp.float32)
        squares = jnp.sum(held_float * held_float, axis=0, keepdims=True)
        tail = jnp.concatenate([squares, squares], axis=0).astype(jnp.bfloat16)
        product = jnp.dot(kernel[...], held, preferred_element_type=jnp.float32)
        product = (product / group_rows + part * direction[...]).astype(jnp.bfloat16)
        for k in range(size):
            at = k * whole_share
            packed[at : at + share, :] = product[k * share : (k + 1) * share, :]
            packed[at + share : at + whole_share, :] = tail

    packed = pl.pallas_call(
        body,
        out_shape=jax.ShapeDtypeStruct((size * whole_share, width), jnp.bfloat16),
        in_specs=[FAST] * 3,
        out_specs=FAST,
        compiler_params=pltpu.CompilerParams(vmem_limit_bytes=8 * 2**20),
        name="returned",
    )(kernel, rounded, direction)
    arrived = exchanged(packed.reshape(size, whole_share // 2, 2, width), axis)
    total = arrived.astype(jnp.float32).sum(axis=0)
    return total[: share // 2].reshape(-1, width), total[share // 2, 0]


def stepped(precond, residual, kernel, older, share):
    centres, rows = kernel.shape
    width = residual.shape[1]
    size = rows // share
    extra = 2 if older is None else 4
    whole_share = share + extra

    def body(precond, residual, kernel, *rest):
        (scaled_out, packed), olds = rest[-2:], rest[:-2]
        held = residual[...]
        scaled = jnp.dot(precond[...], held, preferred_element_type=jnp.float32)
        scaled_out[...] = scaled
        sums = [
            jnp.sum(held.astype(jnp.float32) * scaled, axis=0, keepdims=True),
            jnp.sum(scaled * scaled, axis=0, keepdims=True),
        ]
        for old in olds:
            sums.append(jnp.sum(scaled * old[...], axis=0, keepdims=True))
            sums.append(sums[0])
        tail = jnp.concatenate(sums, axis=0).astype(jnp.bfloat16)
        product = lax.dot_general(
            kernel[...],
            scaled.astype(jnp.bfloat16),
            (((0,), (0,)), ((), ())),
            preferred_element_type=jnp.float32,
        ).astype(jnp.bfloat16)
        for k in range(size):
            at = k * whole_share
            packed[at : at + share, :] = product[k * share : (k + 1) * share, :]
            packed[at + share : at + whole_share, :] = tail

    operands = [precond, residual, kernel] + ([] if older is None else [older])
    scaled, packed = pl.pallas_call(
        body,
        out_shape=[
            jax.ShapeDtypeStruct((centres, width), jnp.float32),
            jax.ShapeDtypeStruct((size * whole_share, width), jnp.bfloat16),
        ],
        in_specs=[FAST] * len(operands),
        out_specs=[FAST] * 2,
        compiler_params=pltpu.CompilerParams(vmem_limit_bytes=8 * 2**20),
        name="stepped",
    )(*operands)
    arrived = exchanged(packed.reshape(size, whole_share // 2, 2, width), ("y", "x"))
    total = arrived.astype(jnp.float32).sum(axis=0)
    sums = [total[share // 2 + i // 2, i % 2] for i in range(2 if older is None else 3)]
    return scaled, total[: share // 2].reshape(-1, width), sums


def finished(row_parts, known, direction, scaled, rows, next_rows, group_rows):

    def body(parts, known, direction, scaled, rows, next_rows, *rest):
        outputs, held, done = rest[:2], rest[2:4], rest[4]
        rows_sq = jnp.sum(parts[...], axis=0, keepdims=True)
        step_size, momentum = known[0:1, :], known[1:2, :]
        next_step = known[2:3, :] / (rows_sq / group_rows + RIDGE_WEIGHT * known[3:4, :])
        copies = [
            pltpu.make_async_copy(held[i], outputs[i], done.at[i]) for i in range(2)
        ]
        both = rows[...].astype(jnp.float32), next_rows[...].astype(jnp.float32)
        held[1][...] = step_size * both[0] + next_step * both[1]
        copies[1].start()
        old = direction[...]
        held[0][...] = step_size * old + next_step * (scaled[...] + momentum * old)
        copies[0].start()
        copies[1].wait()
        copies[0].wait()

    shapes = [
        jax.ShapeDtypeStruct(direction.shape, jnp.float32),
        jax.ShapeDtypeStruct(rows.shape, jnp.float32),
    ]
    return tuple(
        pl.pallas_call(
            body,
            out_shape=shapes,
            in_specs=[FAST] * 6,
            out_specs=[pl.BlockSpec(memory_space=pl.ANY)] * 2,
            scratch_shapes=[pltpu.VMEM(x.shape, x.dtype) for x in shapes]
            + [pltpu.SemaphoreType.DMA((2,))],
            compiler_params=pltpu.CompilerParams(vmem_limit_bytes=4 * 2**20),
            name="finished",
        )(row_parts, known, direction, scaled, rows, next_rows)
    )


def solution(mesh):
    rows, centres = mesh.devices.shape
    split = Mesh(mesh.devices.reshape(rows // 2, 2, centres // 8, 8), ("z", "core", "x", "y"))
    held = ("z", "core")
    plane = ("x", "y")
    return jax.shard_map(
        per_device,
        mesh=split,
        in_specs=(P(held, plane), P(held, None), P(plane, None), P(plane, None)),
        out_specs=(P(plane, None), P(held, None)),
        check_vma=False,
    )
```

```python
import math

import jax
import jax.numpy as jnp
from jax import lax
from jax.experimental import pallas as pl
from jax.experimental.pallas import tpu as pltpu
from jax.sharding import Mesh, PartitionSpec as P

RIDGE_WEIGHT = 0.02
SHARP = 8.0 * math.log2(math.e)
ROWS = ("core", "z")


def exchanged(tiles, axis):
    return lax.all_to_all(tiles, axis, split_axis=0, concat_axis=0, tiled=True)


def copies_of(value, axis):
    copies = jnp.broadcast_to(value, (lax.axis_size(axis), *value.shape))
    return exchanged(copies, axis)


def per_device(features, targets, centre_points, precond):
    group_rows = float(features.shape[0])
    group_parts = copies_of(features.T, "y")
    gathered = copies_of(group_parts, "x").reshape(-1, features.shape[0])
    gathered, centre_points = lax.optimization_barrier((gathered, centre_points))
    kernel, product = built(centre_points, gathered, targets, group_rows)

    def whole(share, axis):
        return copies_of(share.astype(jnp.bfloat16), axis).reshape(-1, share.shape[1])

    def column_sum(a, b):
        return jnp.sum(a * b, axis=0)

    tiles = product.reshape(lax.axis_size(ROWS), -1, product.shape[1])
    residual_share = exchanged(tiles, ROWS).astype(jnp.float32).sum(axis=0)
    residual = whole(residual_share, ROWS)
    share = features.shape[0] // lax.axis_size(("x", "y"))
    direction, rows_share, (product_now, direction_sq) = stepped(
        precond, residual, kernel, None, share
    )
    rounded = whole(rows_share, ("y", "x"))
    applied_share, rows_sq = returned(kernel, rounded, direction, group_rows, ROWS)
    step_size = product_now / (rows_sq / group_rows + RIDGE_WEIGHT * direction_sq)
    residual_share = residual_share - step_size * applied_share
    residual = whole(residual_share, ROWS)
    scaled, scaled_rows_share, (product_next, scaled_sq, cross_term) = stepped(
        precond, residual, kernel, direction, share
    )
    momentum = product_next / product_now
    next_sq = scaled_sq + 2.0 * momentum * cross_term + momentum * momentum * direction_sq
    next_rows_share = scaled_rows_share + momentum * rows_share
    known = jnp.stack([step_size, momentum, product_next, next_sq])
    next_rows_share, known = lax.optimization_barrier((next_rows_share, known))
    next_rows = whole(next_rows_share, ("y", "x"))
    next_parts = column_sum(next_rows.astype(jnp.float32), next_rows.astype(jnp.float32))
    row_parts = copies_of(next_parts[None], ROWS).reshape(-1, next_parts.shape[-1])
    return finished(row_parts, known, direction, scaled, rounded, next_rows, group_rows)


FAST = pl.BlockSpec(memory_space=pltpu.VMEM)


def built(centre_points, gathered, targets, group_rows):
    feature_count, rows = gathered.shape
    centres = centre_points.shape[0]

    def body(centre_points, gathered, targets, kernel, product):
        gathered_float = gathered[...].astype(jnp.float32)
        squares = jnp.sum(gathered_float * gathered_float, axis=0, keepdims=True)
        row_scale = 1.0 / jnp.sqrt(squares / feature_count + 1e-06)
        points = centre_points[...]
        point_float = points.astype(jnp.float32)
        squares = jnp.sum(point_float * point_float, axis=1, keepdims=True)
        centre_scale = (SHARP / feature_count) / jnp.sqrt(squares / feature_count + 1e-06)
        inner = jnp.dot(points, gathered[...], preferred_element_type=jnp.float32)
        values = jnp.exp2(inner * row_scale * centre_scale - SHARP).astype(jnp.bfloat16)
        kernel[...] = values
        part = jnp.dot(values, targets[...], preferred_element_type=jnp.float32)
        product[...] = (part / group_rows**0.5).astype(jnp.bfloat16)

    return pl.pallas_call(
        body,
        out_shape=[
            jax.ShapeDtypeStruct((centres, rows), jnp.bfloat16),
            jax.ShapeDtypeStruct((centres, targets.shape[1]), jnp.bfloat16),
        ],
        in_specs=[FAST] * 3,
        out_specs=[FAST] * 2,
        compiler_params=pltpu.CompilerParams(vmem_limit_bytes=12 * 2**20),
        name="built",
    )(centre_points, gathered, targets)


def returned(kernel, rounded, direction, group_rows, axis):
    size = lax.axis_size(axis)
    centres, width = direction.shape
    share = centres // size
    whole_share = share + 2
    part = RIDGE_WEIGHT / size

    def body(kernel, rounded, direction, packed):
        held = rounded[...]
        held_float = held.astype(jnp.float32)
        squares = jnp.sum(held_float * held_float, axis=0, keepdims=True)
        tail = jnp.concatenate([squares, squares], axis=0).astype(jnp.bfloat16)
        product = jnp.dot(kernel[...], held, preferred_element_type=jnp.float32)
        product = (product / group_rows + part * direction[...]).astype(jnp.bfloat16)
        for k in range(size):
            at = k * whole_share
            packed[at : at + share, :] = product[k * share : (k + 1) * share, :]
            packed[at + share : at + whole_share, :] = tail

    packed = pl.pallas_call(
        body,
        out_shape=jax.ShapeDtypeStruct((size * whole_share, width), jnp.bfloat16),
        in_specs=[FAST] * 3,
        out_specs=FAST,
        compiler_params=pltpu.CompilerParams(vmem_limit_bytes=8 * 2**20),
        name="returned",
    )(kernel, rounded, direction)
    arrived = exchanged(packed.reshape(size, whole_share // 2, 2, width), axis)
    total = arrived.astype(jnp.float32).sum(axis=0)
    return total[: share // 2].reshape(-1, width), total[share // 2, 0]


def stepped(precond, residual, kernel, older, share):
    centres, rows = kernel.shape
    width = residual.shape[1]
    size = rows // share
    extra = 2 if older is None else 4
    whole_share = share + extra

    def body(precond, residual, kernel, *rest):
        (scaled_out, packed), olds = rest[-2:], rest[:-2]
        held = residual[...]
        scaled = jnp.dot(precond[...], held, preferred_element_type=jnp.float32)
        scaled_out[...] = scaled
        sums = [
            jnp.sum(held.astype(jnp.float32) * scaled, axis=0, keepdims=True),
            jnp.sum(scaled * scaled, axis=0, keepdims=True),
        ]
        for old in olds:
            sums.append(jnp.sum(scaled * old[...], axis=0, keepdims=True))
            sums.append(sums[0])
        tail = jnp.concatenate(sums, axis=0).astype(jnp.bfloat16)
        product = lax.dot_general(
            kernel[...],
            scaled.astype(jnp.bfloat16),
            (((0,), (0,)), ((), ())),
            preferred_element_type=jnp.float32,
        ).astype(jnp.bfloat16)
        for k in range(size):
            at = k * whole_share
            packed[at : at + share, :] = product[k * share : (k + 1) * share, :]
            packed[at + share : at + whole_share, :] = tail

    operands = [precond, residual, kernel] + ([] if older is None else [older])
    scaled, packed = pl.pallas_call(
        body,
        out_shape=[
            jax.ShapeDtypeStruct((centres, width), jnp.float32),
            jax.ShapeDtypeStruct((size * whole_share, width), jnp.bfloat16),
        ],
        in_specs=[FAST] * len(operands),
        out_specs=[FAST] * 2,
        compiler_params=pltpu.CompilerParams(vmem_limit_bytes=8 * 2**20),
        name="stepped",
    )(*operands)
    arrived = exchanged(packed.reshape(size, whole_share // 2, 2, width), ("y", "x"))
    total = arrived.astype(jnp.float32).sum(axis=0)
    sums = [total[share // 2 + i // 2, i % 2] for i in range(2 if older is None else 3)]
    return scaled, total[: share // 2].reshape(-1, width), sums


def finished(row_parts, known, direction, scaled, rows, next_rows, group_rows):

    def body(parts, known, direction, scaled, rows, next_rows, *rest):
        outputs, held, done = rest[:2], rest[2:4], rest[4]
        rows_sq = jnp.sum(parts[...], axis=0, keepdims=True)
        step_size, momentum = known[0:1, :], known[1:2, :]
        next_step = known[2:3, :] / (rows_sq / group_rows + RIDGE_WEIGHT * known[3:4, :])
        copies = [
            pltpu.make_async_copy(held[i], outputs[i], done.at[i]) for i in range(2)
        ]
        both = rows[...].astype(jnp.float32), next_rows[...].astype(jnp.float32)
        held[1][...] = step_size * both[0] + next_step * both[1]
        copies[1].start()
        old = direction[...]
        held[0][...] = step_size * old + next_step * (scaled[...] + momentum * old)
        copies[0].start()
        copies[1].wait()
        copies[0].wait()

    shapes = [
        jax.ShapeDtypeStruct(direction.shape, jnp.float32),
        jax.ShapeDtypeStruct(rows.shape, jnp.float32),
    ]
    return tuple(
        pl.pallas_call(
            body,
            out_shape=shapes,
            in_specs=[FAST] * 6,
            out_specs=[pl.BlockSpec(memory_space=pl.ANY)] * 2,
            scratch_shapes=[pltpu.VMEM(x.shape, x.dtype) for x in shapes]
            + [pltpu.SemaphoreType.DMA((2,))],
            compiler_params=pltpu.CompilerParams(vmem_limit_bytes=4 * 2**20),
            name="finished",
        )(row_parts, known, direction, scaled, rows, next_rows)
    )


def solution(mesh):
    rows, centres = mesh.devices.shape
    split = Mesh(mesh.devices.reshape(rows // 2, 2, centres // 8, 8), ("z", "core", "x", "y"))
    held = ("z", "core")
    plane = ("x", "y")
    return jax.shard_map(
        per_device,
        mesh=split,
        in_specs=(P(held, plane), P(held, None), P(plane, None), P(plane, None)),
        out_specs=(P(plane, None), P(held, None)),
        check_vma=False,
    )
```

```python
import math

import jax
import jax.numpy as jnp
from jax import lax
from jax.experimental import pallas as pl
from jax.experimental.pallas import tpu as pltpu
from jax.sharding import Mesh, PartitionSpec as P

RIDGE_WEIGHT = 0.02
SHARP = 8.0 * math.log2(math.e)
ROWS = ("core", "z")


def exchanged(tiles, axis):
    return lax.all_to_all(tiles, axis, split_axis=0, concat_axis=0, tiled=True)


def copies_of(value, axis):
    copies = jnp.broadcast_to(value, (lax.axis_size(axis), *value.shape))
    return exchanged(copies, axis)


def per_device(features, targets, centre_points, precond):
    group_rows = float(features.shape[0])
    group_parts = copies_of(features.T, "y")
    gathered = copies_of(group_parts, "x").reshape(-1, features.shape[0])
    gathered, centre_points = lax.optimization_barrier((gathered, centre_points))
    kernel, product = built(centre_points, gathered, targets, group_rows)

    def whole(share, axis):
        return copies_of(share.astype(jnp.bfloat16), axis).reshape(-1, share.shape[1])

    def column_sum(a, b):
        return jnp.sum(a * b, axis=0)

    tiles = product.reshape(lax.axis_size(ROWS), -1, product.shape[1])
    residual_share = exchanged(tiles, ROWS).astype(jnp.float32).sum(axis=0)
    residual = whole(residual_share, ROWS)
    share = features.shape[0] // lax.axis_size(("x", "y"))
    direction, rows_share, (product_now, direction_sq) = stepped(
        precond, residual, kernel, None, share
    )
    rounded = whole(rows_share, ("y", "x"))
    applied_share, rows_sq = returned(kernel, rounded, direction, group_rows, ROWS)
    step_size = product_now / (rows_sq / group_rows + RIDGE_WEIGHT * direction_sq)
    residual_share = residual_share - step_size * applied_share
    residual = whole(residual_share, ROWS)
    scaled, scaled_rows_share, (product_next, scaled_sq, cross_term) = stepped(
        precond, residual, kernel, direction, share
    )
    momentum = product_next / product_now
    next_sq = scaled_sq + 2.0 * momentum * cross_term + momentum * momentum * direction_sq
    next_rows_share = scaled_rows_share + momentum * rows_share
    known = jnp.stack([step_size, momentum, product_next, next_sq])
    next_rows_share, known = lax.optimization_barrier((next_rows_share, known))
    next_rows = whole(next_rows_share, ("y", "x"))
    next_parts = column_sum(next_rows.astype(jnp.float32), next_rows.astype(jnp.float32))
    row_parts = copies_of(next_parts[None], ROWS).reshape(-1, next_parts.shape[-1])
    return finished(row_parts, known, direction, scaled, rounded, next_rows, group_rows)


FAST = pl.BlockSpec(memory_space=pltpu.VMEM)


def built(centre_points, gathered, targets, group_rows):
    feature_count, rows = gathered.shape
    centres = centre_points.shape[0]
    band = centres // 2

    def body(centre_points, gathered, targets, kernel, product):
        gathered_float = gathered[...].astype(jnp.float32)
        squares = jnp.sum(gathered_float * gathered_float, axis=0, keepdims=True)
        row_scale = 1.0 / jnp.sqrt(squares / feature_count + 1e-06)
        for at in range(0, centres, band):
            points = centre_points[at : at + band, :]
            point_float = points.astype(jnp.float32)
            squares = jnp.sum(point_float * point_float, axis=1, keepdims=True)
            centre_scale = (SHARP / feature_count) / jnp.sqrt(squares / feature_count + 1e-06)
            inner = jnp.dot(points, gathered[...], preferred_element_type=jnp.float32)
            values = jnp.exp2(inner * row_scale * centre_scale - SHARP).astype(jnp.bfloat16)
            kernel[at : at + band, :] = values
            part = jnp.dot(values, targets[...], preferred_element_type=jnp.float32)
            product[at : at + band, :] = (part / group_rows**0.5).astype(jnp.bfloat16)

    return pl.pallas_call(
        body,
        out_shape=[
            jax.ShapeDtypeStruct((centres, rows), jnp.bfloat16),
            jax.ShapeDtypeStruct((centres, targets.shape[1]), jnp.bfloat16),
        ],
        in_specs=[FAST] * 3,
        out_specs=[FAST] * 2,
        compiler_params=pltpu.CompilerParams(vmem_limit_bytes=12 * 2**20),
        name="built",
    )(centre_points, gathered, targets)


def returned(kernel, rounded, direction, group_rows, axis):
    size = lax.axis_size(axis)
    centres, width = direction.shape
    share = centres // size
    whole_share = share + 2
    part = RIDGE_WEIGHT / size

    def body(kernel, rounded, direction, packed):
        held = rounded[...]
        held_float = held.astype(jnp.float32)
        squares = jnp.sum(held_float * held_float, axis=0, keepdims=True)
        tail = jnp.concatenate([squares, squares], axis=0).astype(jnp.bfloat16)
        product = jnp.dot(kernel[...], held, preferred_element_type=jnp.float32)
        product = (product / group_rows + part * direction[...]).astype(jnp.bfloat16)
        for k in range(size):
            at = k * whole_share
            packed[at : at + share, :] = product[k * share : (k + 1) * share, :]
            packed[at + share : at + whole_share, :] = tail

    packed = pl.pallas_call(
        body,
        out_shape=jax.ShapeDtypeStruct((size * whole_share, width), jnp.bfloat16),
        in_specs=[FAST] * 3,
        out_specs=FAST,
        compiler_params=pltpu.CompilerParams(vmem_limit_bytes=8 * 2**20),
        name="returned",
    )(kernel, rounded, direction)
    arrived = exchanged(packed.reshape(size, whole_share // 2, 2, width), axis)
    total = arrived.astype(jnp.float32).sum(axis=0)
    return total[: share // 2].reshape(-1, width), total[share // 2, 0]


def stepped(precond, residual, kernel, older, share):
    centres, rows = kernel.shape
    width = residual.shape[1]
    size = rows // share
    extra = 2 if older is None else 4
    whole_share = share + extra

    def body(precond, residual, kernel, *rest):
        (scaled_out, packed), olds = rest[-2:], rest[:-2]
        held = residual[...]
        scaled = jnp.dot(precond[...], held, preferred_element_type=jnp.float32)
        scaled_out[...] = scaled
        sums = [
            jnp.sum(held.astype(jnp.float32) * scaled, axis=0, keepdims=True),
            jnp.sum(scaled * scaled, axis=0, keepdims=True),
        ]
        for old in olds:
            sums.append(jnp.sum(scaled * old[...], axis=0, keepdims=True))
            sums.append(sums[0])
        tail = jnp.concatenate(sums, axis=0).astype(jnp.bfloat16)
        product = lax.dot_general(
            kernel[...],
            scaled.astype(jnp.bfloat16),
            (((0,), (0,)), ((), ())),
            preferred_element_type=jnp.float32,
        ).astype(jnp.bfloat16)
        for k in range(size):
            at = k * whole_share
            packed[at : at + share, :] = product[k * share : (k + 1) * share, :]
            packed[at + share : at + whole_share, :] = tail

    operands = [precond, residual, kernel] + ([] if older is None else [older])
    scaled, packed = pl.pallas_call(
        body,
        out_shape=[
            jax.ShapeDtypeStruct((centres, width), jnp.float32),
            jax.ShapeDtypeStruct((size * whole_share, width), jnp.bfloat16),
        ],
        in_specs=[FAST] * len(operands),
        out_specs=[FAST] * 2,
        compiler_params=pltpu.CompilerParams(vmem_limit_bytes=8 * 2**20),
        name="stepped",
    )(*operands)
    arrived = exchanged(packed.reshape(size, whole_share // 2, 2, width), ("y", "x"))
    total = arrived.astype(jnp.float32).sum(axis=0)
    sums = [total[share // 2 + i // 2, i % 2] for i in range(2 if older is None else 3)]
    return scaled, total[: share // 2].reshape(-1, width), sums


def finished(row_parts, known, direction, scaled, rows, next_rows, group_rows):

    def body(parts, known, direction, scaled, rows, next_rows, *rest):
        outputs, held, done = rest[:2], rest[2:4], rest[4]
        rows_sq = jnp.sum(parts[...], axis=0, keepdims=True)
        step_size, momentum = known[0:1, :], known[1:2, :]
        next_step = known[2:3, :] / (rows_sq / group_rows + RIDGE_WEIGHT * known[3:4, :])
        copies = [pltpu.make_async_copy(held[0], outputs[0], done.at[0])]
        half = rows.shape[0] // 2
        for i in range(2):
            part = pl.ds(i * half, half)
            both = rows[part, :].astype(jnp.float32), next_rows[part, :].astype(jnp.float32)
            held[1][part, :] = step_size * both[0] + next_step * both[1]
            copies.append(
                pltpu.make_async_copy(
                    held[1].at[part, :], outputs[1].at[part, :], done.at[i + 1]
                )
            )
            copies[-1].start()
        old = direction[...]
        held[0][...] = step_size * old + next_step * (scaled[...] + momentum * old)
        copies[0].start()
        for copy in copies:
            copy.wait()

    shapes = [
        jax.ShapeDtypeStruct(direction.shape, jnp.float32),
        jax.ShapeDtypeStruct(rows.shape, jnp.float32),
    ]
    return tuple(
        pl.pallas_call(
            body,
            out_shape=shapes,
            in_specs=[FAST] * 6,
            out_specs=[pl.BlockSpec(memory_space=pl.ANY)] * 2,
            scratch_shapes=[pltpu.VMEM(x.shape, x.dtype) for x in shapes]
            + [pltpu.SemaphoreType.DMA((3,))],
            compiler_params=pltpu.CompilerParams(vmem_limit_bytes=4 * 2**20),
            name="finished",
        )(row_parts, known, direction, scaled, rows, next_rows)
    )


def solution(mesh):
    rows, centres = mesh.devices.shape
    split = Mesh(mesh.devices.reshape(rows // 2, 2, centres // 8, 8), ("z", "core", "x", "y"))
    held = ("z", "core")
    plane = ("x", "y")
    return jax.shard_map(
        per_device,
        mesh=split,
        in_specs=(P(held, plane), P(held, None), P(plane, None), P(plane, None)),
        out_specs=(P(plane, None), P(held, None)),
        check_vma=False,
    )
```
